16 devices in a mesh: vp: 16 (over z, y, x, core).
Axes of the slice: x: 2, y: 2, z: 2, core: 2. Of those that a mesh axis runs over, the one named last changes fastest.
Arguments:
- residual: bfloat16 [4096, 2048], replicated
- labels: int32 [4096], replicated
- loss_mask: float32 [4096], replicated
- norm_gain: float32 [2048], replicated
- embed_table: bfloat16 [49408, 2048], P('vp')
Outputs:
- output 1: float32 [], replicated
- output 2: float32 [4096, 2048], P('vp')
- output 3: float32 [49408, 2048], P('vp')
- output 4: float32 [2048], replicated
All inputs are finite; a program needn't handle non-finite values.
Results may differ from the reference program's by a relative error of at most 0.001.
Values sent between devices are 32-bit elements.
A program may use at most 1 GiB of HBM per device.

```python
import jax
import jax.numpy as jnp
from jax import lax

TOKENS = 4096
DIM = 2048
VOCAB_REAL = 49155
VOCAB_PAD = 49408

LOGIT_SCALE = 6.0
NORM_EPS = 1e-6


def draw_labels(label_key):
    k_pick, k_wide, k_low = jax.random.split(label_key, 3)
    pick_wide = jax.random.randint(k_pick, (TOKENS,), 0, 2)
    wide_ids = jax.random.randint(k_wide, (TOKENS,), 0, VOCAB_REAL)
    low_ids = jax.random.randint(k_low, (TOKENS,), 0, VOCAB_REAL // 16)
    label_ids = jnp.where(pick_wide == 0, wide_ids, low_ids).astype(jnp.int32)
    return label_ids.at[0].set(0).at[1].set(VOCAB_REAL - 1)


def draw_mask(mask_key):
    keep_draw = jax.random.randint(mask_key, (TOKENS,), 0, 5)
    mask_vals = (keep_draw > 0).astype(jnp.float32)
    return mask_vals.at[0].set(1.0)


def setup_inputs(seed: int = 0) -> dict:
    base_key = jax.random.key(seed)
    k_table, k_noise, k_peak, k_gain, k_label, k_mask = jax.random.split(base_key, 6)
    emb_std = LOGIT_SCALE * DIM ** -0.5
    table_f32 = jax.random.normal(k_table, (VOCAB_PAD, DIM), jnp.float32) * emb_std
    peak_ids = jax.random.randint(k_peak, (TOKENS, 4), 0, VOCAB_REAL)
    peak_sum = jnp.zeros((TOKENS, DIM), jnp.float32)
    for peak in range(4):
        peak_sum = peak_sum + table_f32[peak_ids[:, peak]] / emb_std
    peak_weight = 14.0 * DIM ** -0.5
    noise = jax.random.normal(k_noise, (TOKENS, DIM), jnp.float32)
    residual = (noise + peak_weight * peak_sum).astype(jnp.bfloat16)
    norm_gain = 1.0 + 0.3 * jax.random.normal(k_gain, (DIM,), jnp.float32)
    return {
        'residual': residual,
        'labels': draw_labels(k_label),
        'loss_mask': draw_mask(k_mask),
        'norm_gain': norm_gain,
        'embed_table': table_f32.astype(jnp.bfloat16),
    }


def reference(residual, labels, loss_mask, norm_gain, embed_table):
    x_f32 = residual.astype(jnp.float32)
    inv_rms = lax.rsqrt(jnp.mean(x_f32 * x_f32, axis=-1, keepdims=True) + NORM_EPS)
    x_hat = x_f32 * inv_rms
    hidden = (x_hat * norm_gain).astype(jnp.bfloat16)
    mask_total = jnp.sum(loss_mask)
    tok_weight = loss_mask / mask_total
    col_ids = jnp.arange(VOCAB_PAD)[None, :]
    row_block = min(TOKENS, 256)
    n_blocks = TOKENS // row_block

    def block_step(grad_table, block_in):
        h_blk, lab_blk, w_blk = block_in
        logits = jnp.dot(h_blk, embed_table.T, preferred_element_type=jnp.float32) / LOGIT_SCALE
        logits = jnp.where(col_ids < VOCAB_REAL, logits, -jnp.inf)
        row_max = jnp.max(logits, axis=-1, keepdims=True)
        shifted = jnp.exp(logits - row_max)
        sum_exp = jnp.sum(shifted, axis=-1, keepdims=True)
        is_label = col_ids == lab_blk[:, None]
        target = jnp.sum(jnp.where(is_label, logits, 0.0), axis=-1)
        tok_loss = row_max[:, 0] + jnp.log(sum_exp[:, 0]) - target
        row_prob = shifted / sum_exp
        d_logits = (jnp.where(is_label, row_prob - 1.0, row_prob) * w_blk[:, None]).astype(jnp.bfloat16)
        d_hidden = jnp.dot(d_logits, embed_table, preferred_element_type=jnp.float32) / LOGIT_SCALE
        grad_table = grad_table + jnp.dot(d_logits.T, h_blk, preferred_element_type=jnp.float32) / LOGIT_SCALE
        return grad_table, (tok_loss, d_hidden)

    blocks = (hidden.reshape(n_blocks, row_block, DIM), labels.reshape(n_blocks, row_block), tok_weight.reshape(n_blocks, row_block))
    d_embed, (tok_loss, d_hidden) = lax.scan(block_step, jnp.zeros((VOCAB_PAD, DIM), jnp.float32), blocks)
    tok_loss = tok_loss.reshape(TOKENS)
    d_hidden = d_hidden.reshape(TOKENS, DIM)
    mean_loss = jnp.sum(loss_mask * tok_loss) / mask_total
    d_gain = jnp.sum(d_hidden * x_hat, axis=0)
    d_xhat = d_hidden * norm_gain
    d_residual = inv_rms * (d_xhat - x_hat * jnp.mean(d_xhat * x_hat, axis=-1, keepdims=True))
    return (mean_loss, d_residual, d_embed, d_gain)
```

```python
import functools

import jax
import jax.numpy as jnp
from jax import lax
from jax.experimental import pallas as pl
from jax.experimental.pallas import tpu as pltpu
from jax.sharding import PartitionSpec as P

VOCAB_REAL = 49155
LOGIT_SCALE = 6.0
NORM_EPS = 1e-6
LOG2E = 1.4426950408889634
C2 = LOG2E / LOGIT_SCALE
NEG = -3e38
N_DEV = 16
N_STEP = 8
TC = 512
HALF = 256
LANES = ((0, 768), (768, 640), (1408, 640))
SPLIT = ((2, 1, 0), (1, 0, 2), (0, 2, 1))
N_SND = 3
N_RCV = 4
TB = 32


def flip(i, b):
    return i + b - 2 * b * ((i // b) % 2)


def v_tiles(rows, step):
    n = rows // step
    out = [(i * step, step) for i in range(n)]
    rest = rows - n * step
    if rest:
        out[-1] = (out[-1][0], step + rest)
    return out


def kernel(axis, v_rows, dim,
           x_hbm, lab_ref, maskrow_ref, mask_ref, gain_ref, e_hbm,
           dz_hbm, h_hbm, dx_ref, dg_ref, loss_ref,
           e_ref, z_ref, x_ref, xo_ref, h_ref, dz_ref, dh_ref, d2d_ref, snd_ref, r1_ref, r2_ref, r3_ref,
           st_snd, st_rcv, lse_ref, tgt_ref, dg8_ref, m8_ref, s8_ref, fin_snd, fin_rcv,
           st_ssem, st_rsem, d2d_ssem, d2d_rsem, rs_ssem, rs_rsem, fin_ssem, fin_rsem, lsem):
    me = lax.axis_index(axis)
    chip = me // 2
    core = me % 2
    pos = (chip // 4, (chip // 2) % 2, chip % 2)
    v0 = me * v_rows
    A_TILES = v_tiles(v_rows, 768)

    class Group:
        def __init__(self, copies):
            self.copies = copies

        def start(self):
            for c in self.copies:
                c.start()

        def wait(self):
            for c in self.copies:
                c.wait()

    def x_copy(t):
        return Group([pltpu.make_async_copy(x_hbm.at[:, k, t], x_ref.at[k], lsem.at[k]) for k in range(2)])

    def h_copy(t):
        return pltpu.make_async_copy(h_ref, h_hbm.at[pl.ds(t * TC, TC), :], lsem.at[2])

    def dz_copy(t):
        return pltpu.make_async_copy(dz_ref, dz_hbm.at[:, pl.ds(t * TC, TC)], lsem.at[3])

    def st_copy(t, o):
        return pltpu.make_async_remote_copy(
            src_ref=st_snd.at[t], dst_ref=st_rcv.at[t, me], send_sem=st_ssem.at[o],
            recv_sem=st_rsem.at[t, o], device_id=((me + o) % N_DEV,), device_id_type=pl.DeviceIdType.MESH)

    def d2d_copy(t):
        return pltpu.make_async_remote_copy(
            src_ref=dh_ref.at[0], dst_ref=d2d_ref.at[t % 2], send_sem=d2d_ssem.at[0],
            recv_sem=d2d_rsem.at[t % 2], device_id=(flip(me, 1),), device_id_type=pl.DeviceIdType.MESH)

    def blocks(q, ph, away):
        idx = [slice(None)] * 3
        for i in range(ph):
            idx[SPLIT[q][i]] = pos[SPLIT[q][i]]
        a = SPLIT[q][ph]
        idx[a] = 1 - pos[a] if away else pos[a]
        return tuple(idx)

    def rs_copy(s, q, ph):
        l0, ln = LANES[q]
        lanes = pl.ds(l0, ln)
        src = snd_ref.at[(s % N_SND,) + blocks(q, ph, True) + (slice(None), lanes)]
        rs = s % N_RCV
        dst = (r1_ref.at[rs, :, :, :, lanes], r2_ref.at[rs, :, :, lanes], r3_ref.at[rs, :, lanes])[ph]
        return pltpu.make_async_remote_copy(
            src_ref=src, dst_ref=dst, send_sem=rs_ssem.at[s % N_SND, q, ph], recv_sem=rs_rsem.at[s, q, ph],
            device_id=(flip(me, 8 >> SPLIT[q][ph]),), device_id_type=pl.DeviceIdType.MESH)

    def fin_copy(o):
        return pltpu.make_async_remote_copy(
            src_ref=fin_snd, dst_ref=fin_rcv.at[me], send_sem=fin_ssem.at[o],
            recv_sem=fin_rsem.at[o], device_id=((me + o) % N_DEV,), device_id_type=pl.DeviceIdType.MESH)

    e_copy = pltpu.make_async_copy(e_hbm, e_ref, lsem.at[4])
    xo_copy = pltpu.make_async_copy(x_hbm.at[chip, core], xo_ref, lsem.at[5])
    e_copy.start()
    x_copy(0).start()

    barrier = pltpu.get_barrier_semaphore()
    for o in range(1, N_DEV):
        pl.semaphore_signal(barrier, inc=1, device_id=((me + o) % N_DEV,), device_id_type=pl.DeviceIdType.MESH)
    pl.semaphore_wait(barrier, N_DEV - 1)

    inv_total = 1.0 / jnp.sum(mask_ref[...])
    tgt_ref[...] = jnp.zeros_like(tgt_ref)
    dg8_ref[...] = jnp.zeros_like(dg8_ref)
    gain = gain_ref[...]

    def norm_rows(xv):
        xf = xv.astype(jnp.float32)
        inv = lax.rsqrt(jnp.mean(xf * xf, axis=-1, keepdims=True) + NORM_EPS)
        return xf, inv

    def phase_a(t):
        slot = t % 2
        x_copy(t).wait()

        @pl.when(t > 0)
        def _():
            h_copy(t - 1).wait()

        @pl.loop(0, TC // TB)
        def _(i):
            rows = pl.ds(pl.multiple_of(i * TB, TB), TB)
            xf, inv = norm_rows(x_ref[i // 8, i % 8])
            h_ref[rows, :] = ((xf * inv) * gain).astype(jnp.bfloat16)

        h_copy(t).start()

        @pl.when(t < N_STEP - 1)
        def _():
            x_copy(t + 1).start()

        @pl.when(t == 0)
        def _():
            e_copy.wait()
            xo_copy.start()
            xo_copy.wait()

        m8 = None
        for idx, (r0, rn) in enumerate(A_TILES):
            z = lax.dot_general(e_ref[r0:r0 + rn, :], h_ref[...], (((1,), (1,)), ((), ())),
                                preferred_element_type=jnp.float32)
            if idx == len(A_TILES) - 1:
                rid = lax.broadcasted_iota(jnp.int32, (rn, TC), 0) + (r0 + v0)
                z = jnp.where(rid < VOCAB_REAL, z, NEG)
            z_ref[slot, r0:r0 + rn, :] = z
            zr = z.reshape(rn // 8, 8, TC)
            mt = jnp.max(zr, axis=0)
            if m8 is None:
                mn = mt
                s8 = jnp.sum(jnp.exp2((zr - mn[None]) * C2), axis=0)
            else:
                mn = jnp.maximum(m8, mt)
                s8 = s8 * jnp.exp2((m8 - mn) * C2) + jnp.sum(jnp.exp2((zr - mn[None]) * C2), axis=0)
            m8 = mn
        mx = jnp.max(m8, axis=0, keepdims=True)
        sm = jnp.sum(s8 * jnp.exp2((m8 - mx) * C2), axis=0, keepdims=True)

        @pl.when(t > 0)
        def _():
            for o in range(1, N_DEV):
                st_copy(t - 1, o).wait_send()

        for i in range(4):
            st_snd[t, i:i + 1, :] = mx[:, 128 * i:128 * (i + 1)]
            st_snd[t, 4 + i:5 + i, :] = sm[:, 128 * i:128 * (i + 1)]
        st_rcv[t, me] = st_snd[t]
        for o in range(1, N_DEV):
            st_copy(t, o).start()

    def phase_b(t):
        slot = t % 2
        for o in range(1, N_DEV):
            st_copy(t, o).wait_recv()
        mx = st_rcv[t, 0, 0:4, :]
        for i in range(1, N_DEV):
            mx = jnp.maximum(mx, st_rcv[t, i, 0:4, :])
        sm = jnp.zeros_like(mx)
        for i in range(N_DEV):
            sm = sm + st_rcv[t, i, 4:8, :] * jnp.exp2((st_rcv[t, i, 0:4, :] - mx) * C2)
        lse_ref[t] = mx * (1.0 / LOGIT_SCALE) + jnp.log(sm)
        inv_s = 1.0 / sm
        m8_ref[...] = jnp.concatenate([mx[i:i + 1] for i in range(4)], axis=1)
        s8_ref[...] = jnp.concatenate([inv_s[i:i + 1] for i in range(4)], axis=1)

        @pl.when(t > 0)
        def _():
            dz_copy(t - 1).wait()
            d2d_copy(t - 1).wait_send()

        @pl.loop(0, 2)
        def _(hf):
            off = pl.multiple_of(((hf + 1 + core) % 2) * HALF, HALF)
            cols = pl.ds(off, HALF)
            mrow = m8_ref[:, cols]
            irow = s8_ref[:, cols]
            mk = maskrow_ref[t, :, cols]
            wrow = mk * inv_total
            lab = lab_ref[t, :, cols] - v0
            tg = jnp.zeros((8, HALF), jnp.float32)
            for idx, (r0, rn) in enumerate(A_TILES):
                z = z_ref[slot, r0:r0 + rn, cols]
                p = jnp.exp2((z - mrow) * C2) * irow
                isl = lax.broadcasted_iota(jnp.int32, (rn, HALF), 0) == (lab - r0)
                dz = (jnp.where(isl, p - 1.0, p) * wrow).astype(jnp.bfloat16)
                tg = tg + jnp.sum(jnp.where(isl, z, 0.0).reshape(rn // 8, 8, HALF), axis=0)
                dz_ref[r0:r0 + rn, cols] = dz
                part = lax.dot_general(dz, e_ref[r0:r0 + rn, :], (((0,), (0,)), ((), ())),
                                       preferred_element_type=jnp.float32)
                if idx == 0:
                    dh_ref[hf] = part
                else:
                    dh_ref[hf] += part
            tgt_ref[...] += tg * mk

            @pl.when(hf == 0)
            def _():
                d2d_copy(t).start()

                @pl.when(t > 0)
                def _():
                    rs_advance(t - 1, 1)

        dz_copy(t).start()
        d2d_copy(t).wait_recv()

    def rs_begin(s):
        slot = s % N_SND

        @pl.when(s >= N_SND)
        def _():
            for q in range(3):
                for ph in range(3):
                    rs_copy(s - N_SND, q, ph).wait_send()

        for c in range(8):
            rows = pl.ds(c * TB, TB)
            snd_ref[slot, c // 4, (c // 2) % 2, c % 2] = dh_ref[1, rows, :] + d2d_ref[s % 2, rows, :]
        for q in range(3):
            rs_copy(s, q, 0).start()

    def rs_advance(s, ph):
        slot = s % N_SND
        for q in range(3):
            rs_copy(s, q, ph - 1).wait_recv()
            l0, ln = LANES[q]
            lanes = slice(l0, l0 + ln)
            base = blocks(q, ph - 1, False)
            free = [i for i in range(3) if isinstance(base[i], slice)]
            for n in range(2 ** len(free)):
                bits = [(n >> k) & 1 for k in reversed(range(len(free)))]
                idx = list(base)
                for i, bit in zip(free, bits):
                    idx[i] = bit
                rcv = (r1_ref if ph == 1 else r2_ref)[(s % N_RCV, *bits, slice(None), lanes)]
                loc = (slot, *idx, slice(None), lanes)
                snd_ref[loc] = snd_ref[loc] + rcv
            rs_copy(s, q, ph).start()

    def rs_finish(s):
        for q in range(3):
            rs_copy(s, q, 2).wait_recv()

        @pl.loop(0, TB // 8)
        def _(i):
            rows = pl.ds(pl.multiple_of(i * 8, 8), 8)
            acc = (snd_ref[s % N_SND, pos[0], pos[1], pos[2], rows, :] + r3_ref[s % N_RCV, rows, :]) * (1.0 / LOGIT_SCALE)
            xf, inv = norm_rows(xo_ref[s, rows, :])
            xh = xf * inv
            u = acc * gain
            dx_ref[pl.ds(pl.multiple_of(s * TB + i * 8, 8), 8), :] = inv * (
                u - xh * jnp.mean(u * xh, axis=-1, keepdims=True))
            dg8_ref[...] += acc * xh

    @pl.loop(0, N_STEP + 1)
    def _(t):
        @pl.when(t < N_STEP)
        def _():
            phase_a(t)

        @pl.when(t > 3)
        def _():
            rs_finish(t - 4)

        @pl.when(t > 2)
        def _():
            rs_advance(t - 3, 2)

        @pl.when(t > 0)
        def _():
            phase_b(t - 1)
            rs_begin(t - 1)

    rs_finish(N_STEP - 3)
    rs_advance(N_STEP - 2, 2)
    rs_advance(N_STEP - 1, 1)
    rs_finish(N_STEP - 2)
    rs_advance(N_STEP - 1, 2)
    rs_finish(N_STEP - 1)

    dg = jnp.sum(dg8_ref[...], axis=0, keepdims=True)
    for i in range(dim // 128):
        fin_snd[i:i + 1, :] = dg[:, 128 * i:128 * (i + 1)]
    tg = jnp.sum(tgt_ref[...], axis=0, keepdims=True)
    fin_snd[16:24, :] = jnp.broadcast_to(tg[:, 0:128] + tg[:, 128:256], (8, 128))
    fin_rcv[me] = fin_snd[...]
    for o in range(1, N_DEV):
        fin_copy(o).start()
    for o in range(1, N_DEV):
        st_copy(N_STEP - 1, o).wait_send()
        fin_copy(o).wait()
    tot = fin_rcv[0]
    for i in range(1, N_DEV):
        tot = tot + fin_rcv[i]
    dg_ref[...] = tot[0:16, :]
    lse_sum = jnp.sum(mask_ref[...] * lse_ref[...])
    tgt_sum = jnp.sum(tot[16:17, :]) * (1.0 / LOGIT_SCALE)
    loss_ref[...] = jnp.broadcast_to((lse_sum - tgt_sum) * inv_total, loss_ref.shape)

    for s in range(N_STEP - N_SND, N_STEP):
        for q in range(3):
            for ph in range(3):
                rs_copy(s, q, ph).wait_send()
    h_copy(N_STEP - 1).wait()
    dz_copy(N_STEP - 1).wait()
    d2d_copy(N_STEP - 1).wait_send()


def solution(mesh):
    axis = mesh.axis_names[0]

    def local_step(residual, labels, loss_mask, norm_gain, table_shard):
        tokens, dim = residual.shape
        v_rows = table_shard.shape[0]
        by_step = lambda a: a.reshape(8, 2, N_STEP, TB).transpose(2, 1, 0, 3)
        any_spec = pl.BlockSpec(memory_space=pl.ANY)
        vmem = pl.BlockSpec(memory_space=pltpu.VMEM)
        f32, bf16 = jnp.float32, jnp.bfloat16
        dma = pltpu.SemaphoreType.DMA
        dz, h, dx, dg, loss = pl.pallas_call(
            functools.partial(kernel, axis, v_rows, dim),
            out_shape=(
                jax.ShapeDtypeStruct((v_rows, tokens), bf16),
                jax.ShapeDtypeStruct((tokens, dim), bf16),
                jax.ShapeDtypeStruct((HALF, dim), f32),
                jax.ShapeDtypeStruct((16, 128), f32),
                jax.ShapeDtypeStruct((8, 128), f32),
            ),
            in_specs=[any_spec, vmem, vmem, vmem, vmem, any_spec],
            out_specs=(any_spec, any_spec, vmem, vmem, vmem),
            scratch_shapes=[
                pltpu.VMEM((v_rows, dim), bf16),
                pltpu.VMEM((2, v_rows, TC), f32),
                pltpu.VMEM((2, 8, TB, dim), bf16),
                pltpu.VMEM((N_STEP, TB, dim), bf16),
                pltpu.VMEM((TC, dim), bf16),
                pltpu.VMEM((v_rows, TC), bf16),
                pltpu.VMEM((2, HALF, dim), f32),
                pltpu.VMEM((2, HALF, dim), f32),
                pltpu.VMEM((N_SND, 2, 2, 2, TB, dim), f32),
                pltpu.VMEM((N_RCV, 2, 2, TB, dim), f32),
                pltpu.VMEM((N_RCV, 2, TB, dim), f32),
                pltpu.VMEM((N_RCV, TB, dim), f32),
                pltpu.VMEM((N_STEP, 8, 128), f32),
                pltpu.VMEM((N_STEP, N_DEV, 8, 128), f32),
                pltpu.VMEM((N_STEP, 4, 128), f32),
                pltpu.VMEM((8, HALF), f32),
                pltpu.VMEM((8, dim), f32),
                pltpu.VMEM((1, TC), f32),
                pltpu.VMEM((1, TC), f32),
                pltpu.VMEM((24, 128), f32),
                pltpu.VMEM((N_DEV, 24, 128), f32),
                dma((N_DEV,)), dma((N_STEP, N_DEV)), dma((1,)), dma((2,)),
                dma((N_SND, 3, 3)), dma((N_STEP, 3, 3)), dma((N_DEV,)), dma((N_DEV,)), dma((6,)),
            ],
            compiler_params=pltpu.CompilerParams(
                collective_id=0, has_side_effects=True, vmem_limit_bytes=67043328),
            name="xent_fused",
        )(residual.reshape(8, 2, N_STEP, TB, dim), by_step(labels).reshape(N_STEP, 1, TC),
          by_step(loss_mask).reshape(N_STEP, 1, TC), by_step(loss_mask).reshape(N_STEP, 4, 128),
          norm_gain.reshape(1, dim), table_shard)
        d_embed = jnp.dot(dz, h, preferred_element_type=f32) / LOGIT_SCALE
        return loss[0, 0], dx, d_embed, dg.reshape(dim)

    return jax.shard_map(local_step, mesh=mesh, in_specs=(P(), P(), P(), P(), P(axis, None)),
                         out_specs=(P(), P(axis, None), P(axis, None), P()), check_vma=False)
```

```python
import functools

import jax
import jax.numpy as jnp
from jax import lax
from jax.experimental import pallas as pl
from jax.experimental.pallas import tpu as pltpu
from jax.sharding import PartitionSpec as P

VOCAB_REAL = 49155
LOGIT_SCALE = 6.0
NORM_EPS = 1e-6
LOG2E = 1.4426950408889634
C2 = LOG2E / LOGIT_SCALE
NEG = -3e38
N_DEV = 16
N_STEP = 8
TC = 512
HALF = 256
LANES = ((0, 768), (768, 640), (1408, 640))
SPLIT = ((2, 1, 0), (1, 0, 2), (0, 2, 1))
N_SND = 3
N_RCV = 4
TB = 32
N_XLA = 5


def flip(i, b):
    return i + b - 2 * b * ((i // b) % 2)


def v_tiles(rows, step):
    n = rows // step
    out = [(i * step, step) for i in range(n)]
    rest = rows - n * step
    if rest:
        out[-1] = (out[-1][0], step + rest)
    return out


def kernel(axis, v_rows, dim,
           x_hbm, lab_ref, maskrow_ref, mask_ref, gain_ref, e_hbm,
           dz_hbm, h_hbm, dzt_hbm, ht_hbm, part_hbm, dx_ref, dg_ref, loss_ref,
           e_ref, z_ref, x_ref, xo_ref, h_ref, dz_ref, dh_ref, d2d_ref, snd_ref, r1_ref, r2_ref, r3_ref,
           st_snd, st_rcv, lse_ref, tgt_ref, dg8_ref, m8_ref, s8_ref, fin_snd, fin_rcv,
           st_ssem, st_rsem, d2d_ssem, d2d_rsem, rs_ssem, rs_rsem, fin_ssem, fin_rsem, lsem):
    me = lax.axis_index(axis)
    chip = me // 2
    core = me % 2
    pos = (chip // 4, (chip // 2) % 2, chip % 2)
    v0 = me * v_rows
    A_TILES = v_tiles(v_rows, 384)
    B_TILES = v_tiles(v_rows, 768)

    class Group:
        def __init__(self, copies):
            self.copies = copies

        def start(self):
            for c in self.copies:
                c.start()

        def wait(self):
            for c in self.copies:
                c.wait()

    def x_copy(t):
        return Group([pltpu.make_async_copy(x_hbm.at[:, k, t], x_ref.at[k], lsem.at[k]) for k in range(2)])

    def h_copy(t):
        return pltpu.make_async_copy(h_ref.at[t % 2], h_hbm.at[t], lsem.at[8 + t % 2])

    def dz_copy(t):
        return pltpu.make_async_copy(dz_ref, dz_hbm.at[:, pl.ds(pl.multiple_of(t * TC, TC), TC)], lsem.at[3])

    def ht_copy():
        return pltpu.make_async_copy(h_ref.at[N_XLA % 2], ht_hbm, lsem.at[8 + N_XLA % 2])

    def dzt_copy(t):
        return pltpu.make_async_copy(dz_ref, dzt_hbm.at[t - N_XLA], lsem.at[3])

    def dz_save(t):
        @pl.when(t < N_XLA)
        def _():
            dz_copy(t).start()

        @pl.when((t >= N_XLA) & (t < N_STEP - 1))
        def _():
            dzt_copy(t).start()

    def dz_save_wait(t):
        @pl.when(t < N_XLA)
        def _():
            dz_copy(t).wait()

        @pl.when(t >= N_XLA)
        def _():
            dzt_copy(t).wait()

    def part_copy(n):
        return pltpu.make_async_copy(
            z_ref.at[n % 2], part_hbm.at[:, pl.ds(pl.multiple_of(n * TC, TC), TC)], lsem.at[6 + n % 2])

    def st_copy(t, o):
        return pltpu.make_async_remote_copy(
            src_ref=st_snd.at[t], dst_ref=st_rcv.at[t, me], send_sem=st_ssem.at[o],
            recv_sem=st_rsem.at[t, o], device_id=((me + o) % N_DEV,), device_id_type=pl.DeviceIdType.MESH)

    def d2d_copy(t):
        return pltpu.make_async_remote_copy(
            src_ref=dh_ref.at[0], dst_ref=d2d_ref.at[t % 2], send_sem=d2d_ssem.at[0],
            recv_sem=d2d_rsem.at[t % 2], device_id=(flip(me, 1),), device_id_type=pl.DeviceIdType.MESH)

    def blocks(q, ph, away):
        idx = [slice(None)] * 3
        for i in range(ph):
            idx[SPLIT[q][i]] = pos[SPLIT[q][i]]
        a = SPLIT[q][ph]
        idx[a] = 1 - pos[a] if away else pos[a]
        return tuple(idx)

    def rs_copy(s, q, ph):
        l0, ln = LANES[q]
        lanes = pl.ds(l0, ln)
        src = snd_ref.at[(s % N_SND,) + blocks(q, ph, True) + (slice(None), lanes)]
        rs = s % N_RCV
        dst = (r1_ref.at[rs, :, :, :, lanes], r2_ref.at[rs, :, :, lanes], r3_ref.at[rs, :, lanes])[ph]
        return pltpu.make_async_remote_copy(
            src_ref=src, dst_ref=dst, send_sem=rs_ssem.at[s % N_SND, q, ph], recv_sem=rs_rsem.at[s, q, ph],
            device_id=(flip(me, 8 >> SPLIT[q][ph]),), device_id_type=pl.DeviceIdType.MESH)

    def fin_copy(o):
        return pltpu.make_async_remote_copy(
            src_ref=fin_snd, dst_ref=fin_rcv.at[me], send_sem=fin_ssem.at[o],
            recv_sem=fin_rsem.at[o], device_id=((me + o) % N_DEV,), device_id_type=pl.DeviceIdType.MESH)

    e_copy = pltpu.make_async_copy(e_hbm, e_ref, lsem.at[4])
    xo_copy = pltpu.make_async_copy(x_hbm.at[chip, core], xo_ref, lsem.at[5])
    e_copy.start()
    x_copy(0).start()

    barrier = pltpu.get_barrier_semaphore()
    for o in range(1, N_DEV):
        pl.semaphore_signal(barrier, inc=1, device_id=((me + o) % N_DEV,), device_id_type=pl.DeviceIdType.MESH)

    inv_total = 1.0 / jnp.sum(mask_ref[...])
    tgt_ref[...] = jnp.zeros_like(tgt_ref)
    dg8_ref[...] = jnp.zeros_like(dg8_ref)
    gain = gain_ref[...]

    def norm_rows(xv):
        xf = xv.astype(jnp.float32)
        inv = lax.rsqrt(jnp.mean(xf * xf, axis=-1, keepdims=True) + NORM_EPS)
        return xf, inv

    def norm_block(slot, k, c):
        xf, inv = norm_rows(x_ref[k, c])
        h_ref[slot, k, c] = ((xf * inv) * gain).astype(jnp.bfloat16)

    for t in range(2):
        x_copy(t).wait()

        @pl.loop(0, TC // TB)
        def _(i, t=t):
            norm_block(t, i // 8, i % 8)

        if t == 0:
            x_copy(1).start()
            xo_copy.start()
    xo_copy.wait()
    pl.semaphore_wait(barrier, N_DEV - 1)
    e_copy.wait()

    def phase_a(t):
        slot = t % 2
        @pl.when(t < N_XLA)
        def _():
            h_copy(t).start()

        @pl.when(t == N_XLA)
        def _():
            ht_copy().start()

        @pl.when((t > 0) & (t < N_STEP - 1))
        def _():
            x_copy(t + 1).start()

        h_val = h_ref[t % 2].reshape(TC, dim)
        m8 = None
        for idx, (r0, rn) in enumerate(A_TILES):
            z = lax.dot_general(e_ref[r0:r0 + rn, :], h_val, (((1,), (1,)), ((), ())),
                                preferred_element_type=jnp.float32)
            if idx == len(A_TILES) - 1:
                rid = lax.broadcasted_iota(jnp.int32, (rn, TC), 0) + (r0 + v0)
                z = jnp.where(rid < VOCAB_REAL, z, NEG)
            z_ref[slot, r0:r0 + rn, :] = z
            zr = z.reshape(rn // 8, 8, TC)
            mt = jnp.max(zr, axis=0)
            if m8 is None:
                mn = mt
                s8 = jnp.sum(jnp.exp2((zr - mn[None]) * C2), axis=0)
            else:
                mn = jnp.maximum(m8, mt)
                s8 = s8 * jnp.exp2((m8 - mn) * C2) + jnp.sum(jnp.exp2((zr - mn[None]) * C2), axis=0)
            m8 = mn
        mx = jnp.max(m8, axis=0, keepdims=True)
        sm = jnp.sum(s8 * jnp.exp2((m8 - mx) * C2), axis=0, keepdims=True)

        @pl.when(t > 0)
        def _():
            for o in range(1, N_DEV):
                st_copy(t - 1, o).wait_send()

        for i in range(4):
            st_snd[t, i:i + 1, :] = mx[:, 128 * i:128 * (i + 1)]
            st_snd[t, 4 + i:5 + i, :] = sm[:, 128 * i:128 * (i + 1)]
        st_rcv[t, me] = st_snd[t]
        for o in range(1, N_DEV):
            st_copy(t, o).start()

    def phase_b(t):
        slot = t % 2
        for o in range(1, N_DEV):
            st_copy(t, o).wait_recv()
        mx = st_rcv[t, 0, 0:4, :]
        for i in range(1, N_DEV):
            mx = jnp.maximum(mx, st_rcv[t, i, 0:4, :])
        sm = jnp.zeros_like(mx)
        for i in range(N_DEV):
            sm = sm + st_rcv[t, i, 4:8, :] * jnp.exp2((st_rcv[t, i, 0:4, :] - mx) * C2)
        lse_ref[t] = mx * (1.0 / LOGIT_SCALE) + jnp.log(sm)
        inv_s = 1.0 / sm
        m8_ref[...] = jnp.concatenate([mx[i:i + 1] for i in range(4)], axis=1)
        s8_ref[...] = jnp.concatenate([inv_s[i:i + 1] for i in range(4)], axis=1)

        @pl.when(t > 0)
        def _():
            dz_save_wait(t - 1)
            d2d_copy(t - 1).wait_send()

        @pl.when(t < N_XLA)
        def _():
            h_copy(t).wait()

        @pl.when(t == N_XLA)
        def _():
            ht_copy().wait()

        @pl.when(t < N_STEP - 2)
        def _():
            x_copy(t + 2).wait()

        spare = (t + 2) // N_STEP
        h_slot = (t % 2) * (1 - spare) + 2 * spare

        @pl.loop(0, 2)
        def _(hf):
            off = pl.multiple_of(((hf + 1 + core) % 2) * HALF, HALF)
            cols = pl.ds(off, HALF)
            mrow = m8_ref[:, cols]
            irow = s8_ref[:, cols]
            mk = maskrow_ref[t, :, cols]
            wrow = mk * inv_total
            lab = lab_ref[t, :, cols] - v0
            tg = jnp.zeros((8, HALF), jnp.float32)
            for idx, (r0, rn) in enumerate(B_TILES):
                z = z_ref[slot, r0:r0 + rn, cols]
                p = jnp.exp2((z - mrow) * C2) * irow
                isl = lax.broadcasted_iota(jnp.int32, (rn, HALF), 0) == (lab - r0)
                dz = (jnp.where(isl, p - 1.0, p) * wrow).astype(jnp.bfloat16)
                tg = tg + jnp.sum(jnp.where(isl, z, 0.0).reshape(rn // 8, 8, HALF), axis=0)
                dz_ref[r0:r0 + rn, cols] = dz
                for c in range(8 * idx // len(B_TILES), 8 * (idx + 1) // len(B_TILES)):
                    norm_block(h_slot, hf, c)
                part = lax.dot_general(dz, e_ref[r0:r0 + rn, :], (((0,), (0,)), ((), ())),
                                       preferred_element_type=jnp.float32)
                if idx == 0:
                    dh_ref[hf] = part
                else:
                    dh_ref[hf] += part
            tgt_ref[...] += tg * mk

            @pl.when(hf == 0)
            def _():
                d2d_copy(t).start()

                @pl.when(t > 0)
                def _():
                    rs_advance(t - 1, 1)

        dz_save(t)
        d2d_copy(t).wait_recv()

    def rs_begin(s):
        slot = s % N_SND

        @pl.when(s >= N_SND)
        def _():
            for q in range(3):
                for ph in range(3):
                    rs_copy(s - N_SND, q, ph).wait_send()

        for c in range(8):
            rows = pl.ds(c * TB, TB)
            snd_ref[slot, c // 4, (c // 2) % 2, c % 2] = dh_ref[1, rows, :] + d2d_ref[s % 2, rows, :]
        for q in range(3):
            rs_copy(s, q, 0).start()

    def rs_advance(s, ph):
        slot = s % N_SND
        for q in range(3):
            rs_copy(s, q, ph - 1).wait_recv()
            l0, ln = LANES[q]
            lanes = slice(l0, l0 + ln)
            base = blocks(q, ph - 1, False)
            free = [i for i in range(3) if isinstance(base[i], slice)]
            for n in range(2 ** len(free)):
                bits = [(n >> k) & 1 for k in reversed(range(len(free)))]
                idx = list(base)
                for i, bit in zip(free, bits):
                    idx[i] = bit
                rcv = (r1_ref if ph == 1 else r2_ref)[(s % N_RCV, *bits, slice(None), lanes)]
                loc = (slot, *idx, slice(None), lanes)
                snd_ref[loc] = snd_ref[loc] + rcv
            rs_copy(s, q, ph).start()

    def rs_finish(s):
        for q in range(3):
            rs_copy(s, q, 2).wait_recv()

        @pl.loop(0, TB // 8)
        def _(i):
            rows = pl.ds(pl.multiple_of(i * 8, 8), 8)
            acc = (snd_ref[s % N_SND, pos[0], pos[1], pos[2], rows, :] + r3_ref[s % N_RCV, rows, :]) * (1.0 / LOGIT_SCALE)
            xf, inv = norm_rows(xo_ref[s, rows, :])
            xh = xf * inv
            u = acc * gain
            dx_ref[pl.ds(pl.multiple_of(s * TB + i * 8, 8), 8), :] = inv * (
                u - xh * jnp.mean(u * xh, axis=-1, keepdims=True))
            dg8_ref[...] += acc * xh

    @pl.loop(0, N_STEP + 1)
    def _(t):
        @pl.when(t < N_STEP)
        def _():
            phase_a(t)

        @pl.when(t > 3)
        def _():
            rs_finish(t - 4)

        @pl.when(t > 2)
        def _():
            rs_advance(t - 3, 2)

        @pl.when(t > 0)
        def _():
            phase_b(t - 1)
            rs_begin(t - 1)

    loads = [pltpu.make_async_copy(dzt_hbm.at[i], e_ref.at[:, i * TC:(i + 1) * TC], lsem.at[i]) for i in range(2)]
    loads.append(pltpu.make_async_copy(ht_hbm, x_ref, lsem.at[2]))
    for c in loads:
        c.start()
    rs_finish(N_STEP - 3)
    rs_advance(N_STEP - 2, 2)
    for c in loads:
        c.wait()

    @pl.loop(0, dim // TC)
    def _(n):
        @pl.when(n > 1)
        def _():
            part_copy(n - 2).wait()

        cols = pl.ds(pl.multiple_of(n * TC, TC), TC)
        for r0, rn in A_TILES:
            acc = None
            for lhs, rhs in ((dz_ref[r0:r0 + rn, :], h_ref[(N_STEP - 1) % 2, :, :, :, cols]),
                             (e_ref[r0:r0 + rn, TC:2 * TC], h_ref[(N_STEP - 2) % 2, :, :, :, cols]),
                             (e_ref[r0:r0 + rn, 0:TC], x_ref[:, :, :, cols])):
                part = jnp.dot(lhs, rhs.reshape(TC, TC), preferred_element_type=jnp.float32)
                acc = part if acc is None else acc + part
            z_ref[n % 2, r0:r0 + rn, :] = acc
        part_copy(n).start()

        @pl.when(n == 1)
        def _():
            rs_advance(N_STEP - 1, 1)
            rs_finish(N_STEP - 2)

        @pl.when(n == 2)
        def _():
            rs_advance(N_STEP - 1, 2)

    rs_finish(N_STEP - 1)

    dg = jnp.sum(dg8_ref[...], axis=0, keepdims=True)
    for i in range(dim // 128):
        fin_snd[i:i + 1, :] = dg[:, 128 * i:128 * (i + 1)]
    tg = jnp.sum(tgt_ref[...], axis=0, keepdims=True)
    fin_snd[16:24, :] = jnp.broadcast_to(tg[:, 0:128] + tg[:, 128:256], (8, 128))
    fin_rcv[me] = fin_snd[...]
    for o in range(1, N_DEV):
        fin_copy(o).start()
    for o in range(1, N_DEV):
        st_copy(N_STEP - 1, o).wait_send()
        fin_copy(o).wait()
    tot = fin_rcv[0]
    for i in range(1, N_DEV):
        tot = tot + fin_rcv[i]
    dg_ref[...] = tot[0:16, :]
    lse_sum = jnp.sum(mask_ref[...] * lse_ref[...])
    tgt_sum = jnp.sum(tot[16:17, :]) * (1.0 / LOGIT_SCALE)
    loss_ref[...] = jnp.broadcast_to((lse_sum - tgt_sum) * inv_total, loss_ref.shape)

    for s in range(N_STEP - N_SND, N_STEP):
        for q in range(3):
            for ph in range(3):
                rs_copy(s, q, ph).wait_send()
    part_copy(2).wait()
    part_copy(3).wait()
    d2d_copy(N_STEP - 1).wait_send()


def solution(mesh):
    axis = mesh.axis_names[0]

    def local_step(residual, labels, loss_mask, norm_gain, table_shard):
        tokens, dim = residual.shape
        v_rows = table_shard.shape[0]
        by_step = lambda a: a.reshape(8, 2, N_STEP, TB).transpose(2, 1, 0, 3)
        any_spec = pl.BlockSpec(memory_space=pl.ANY)
        vmem = pl.BlockSpec(memory_space=pltpu.VMEM)
        f32, bf16 = jnp.float32, jnp.bfloat16
        dma = pltpu.SemaphoreType.DMA
        dz, h, _, _, part, dx, dg, loss = pl.pallas_call(
            functools.partial(kernel, axis, v_rows, dim),
            out_shape=(
                jax.ShapeDtypeStruct((v_rows, N_XLA * TC), bf16),
                jax.ShapeDtypeStruct((N_XLA, 2, 8, TB, dim), bf16),
                jax.ShapeDtypeStruct((2, v_rows, TC), bf16),
                jax.ShapeDtypeStruct((2, 8, TB, dim), bf16),
                jax.ShapeDtypeStruct((v_rows, dim), f32),
                jax.ShapeDtypeStruct((HALF, dim), f32),
                jax.ShapeDtypeStruct((16, 128), f32),
                jax.ShapeDtypeStruct((8, 128), f32),
            ),
            in_specs=[any_spec, vmem, vmem, vmem, vmem, any_spec],
            out_specs=(any_spec, any_spec, any_spec, any_spec, any_spec, vmem, vmem, vmem),
            scratch_shapes=[
                pltpu.VMEM((v_rows, dim), bf16),
                pltpu.VMEM((2, v_rows, TC), f32),
                pltpu.VMEM((2, 8, TB, dim), bf16),
                pltpu.VMEM((N_STEP, TB, dim), bf16),
                pltpu.VMEM((3, 2, 8, TB, dim), bf16),
                pltpu.VMEM((v_rows, TC), bf16),
                pltpu.VMEM((2, HALF, dim), f32),
                pltpu.VMEM((2, HALF, dim), f32),
                pltpu.VMEM((N_SND, 2, 2, 2, TB, dim), f32),
                pltpu.VMEM((N_RCV, 2, 2, TB, dim), f32),
                pltpu.VMEM((N_RCV, 2, TB, dim), f32),
                pltpu.VMEM((N_RCV, TB, dim), f32),
                pltpu.VMEM((N_STEP, 8, 128), f32),
                pltpu.VMEM((N_STEP, N_DEV, 8, 128), f32),
                pltpu.VMEM((N_STEP, 4, 128), f32),
                pltpu.VMEM((8, HALF), f32),
                pltpu.VMEM((8, dim), f32),
                pltpu.VMEM((1, TC), f32),
                pltpu.VMEM((1, TC), f32),
                pltpu.VMEM((24, 128), f32),
                pltpu.VMEM((N_DEV, 24, 128), f32),
                dma((N_DEV,)), dma((N_STEP, N_DEV)), dma((1,)), dma((2,)),
                dma((N_SND, 3, 3)), dma((N_STEP, 3, 3)), dma((N_DEV,)), dma((N_DEV,)), dma((10,)),
            ],
            compiler_params=pltpu.CompilerParams(
                collective_id=0, has_side_effects=True, vmem_limit_bytes=67043328),
            name="xent_fused",
        )(residual.reshape(8, 2, N_STEP, TB, dim), by_step(labels).reshape(N_STEP, 1, TC),
          by_step(loss_mask).reshape(N_STEP, 1, TC), by_step(loss_mask).reshape(N_STEP, 4, 128),
          norm_gain.reshape(1, dim), table_shard)
        d_embed = (jnp.dot(dz, h.reshape(N_XLA * TC, dim), preferred_element_type=f32) + part) / LOGIT_SCALE
        return loss[0, 0], dx, d_embed, dg.reshape(dim)

    return jax.shard_map(local_step, mesh=mesh, in_specs=(P(), P(), P(), P(), P(axis, None)),
                         out_specs=(P(), P(axis, None), P(axis, None), P()), check_vma=False)
```

```python
import functools

import jax
import jax.numpy as jnp
from jax import lax
from jax.experimental import pallas as pl
from jax.experimental.pallas import tpu as pltpu
from jax.sharding import PartitionSpec as P

VOCAB_REAL = 49155
LOGIT_SCALE = 6.0
NORM_EPS = 1e-6
LOG2E = 1.4426950408889634
C2 = LOG2E / LOGIT_SCALE
NEG = -3e38
N_DEV = 16
N_STEP = 8
TC = 512
HALF = 256
LANES = ((0, 768), (768, 640), (1408, 640))
SPLIT = ((2, 1, 0), (1, 0, 2), (0, 2, 1))
N_SND = 3
N_RCV = 4
TB = 32
N_XLA = 5
PAD = 128


def flip(i, b):
    return i + b - 2 * b * ((i // b) % 2)


def v_tiles(rows, step):
    n = rows // step
    out = [(i * step, step) for i in range(n)]
    rest = rows - n * step
    if rest:
        out[-1] = (out[-1][0], step + rest)
    return out


def kernel(axis, v_rows, dim,
           x_hbm, lab_ref, gain_ref, e_hbm,
           dz_hbm, h_hbm, dzt_hbm, ht_hbm, part_hbm, dx_ref, dg_ref, loss_ref,
           e_ref, z_ref, x_ref, xo_ref, h_ref, dz_ref, dh_ref, d2d_ref, snd_ref, r1_ref, r2_ref, r3_ref,
           st_snd, st_rcv, lse_ref, tgt_ref, dg8_ref, m8_ref, s8_ref, fin_snd, fin_rcv,
           st_ssem, st_rsem, d2d_ssem, d2d_rsem, rs_ssem, rs_rsem, fin_ssem, fin_rsem, lsem):
    me = lax.axis_index(axis)
    chip = me // 2
    core = me % 2
    pos = (chip // 4, (chip // 2) % 2, chip % 2)
    v0 = me * v_rows
    A_TILES = v_tiles(v_rows, 384)
    B_TILES = v_tiles(v_rows, 768)

    class Group:
        def __init__(self, copies):
            self.copies = copies

        def start(self):
            for c in self.copies:
                c.start()

        def wait(self):
            for c in self.copies:
                c.wait()

    def x_copy(t):
        return Group([pltpu.make_async_copy(x_hbm.at[:, k, t], x_ref.at[k], lsem.at[k]) for k in range(2)])

    def h_copy(t):
        return pltpu.make_async_copy(h_ref.at[t % 2], h_hbm.at[t], lsem.at[8 + t % 2])

    def dz_copy(t):
        return pltpu.make_async_copy(dz_ref, dz_hbm.at[:, pl.ds(pl.multiple_of(t * TC, TC), TC)], lsem.at[3])

    def ht_copy():
        return pltpu.make_async_copy(h_ref.at[N_XLA % 2], ht_hbm, lsem.at[8 + N_XLA % 2])

    def dzt_copy(t):
        return pltpu.make_async_copy(dz_ref, dzt_hbm.at[t - N_XLA], lsem.at[3])

    def dz_save(t):
        @pl.when(t < N_XLA)
        def _():
            dz_copy(t).start()

        @pl.when((t >= N_XLA) & (t < N_STEP - 1))
        def _():
            dzt_copy(t).start()

    def dz_save_wait(t):
        @pl.when(t < N_XLA)
        def _():
            dz_copy(t).wait()

        @pl.when(t >= N_XLA)
        def _():
            dzt_copy(t).wait()

    def part_copy(n):
        return pltpu.make_async_copy(
            z_ref.at[n % 2], part_hbm.at[:, pl.ds(pl.multiple_of(n * TC, TC), TC)], lsem.at[6 + n % 2])

    def st_copy(t, o):
        return pltpu.make_async_remote_copy(
            src_ref=st_snd.at[t], dst_ref=st_rcv.at[t, me], send_sem=st_ssem.at[o],
            recv_sem=st_rsem.at[t, o], device_id=((me + o) % N_DEV,), device_id_type=pl.DeviceIdType.MESH)

    def d2d_copy(t):
        return pltpu.make_async_remote_copy(
            src_ref=dh_ref.at[0], dst_ref=d2d_ref.at[t % 2], send_sem=d2d_ssem.at[0],
            recv_sem=d2d_rsem.at[t % 2], device_id=(flip(me, 1),), device_id_type=pl.DeviceIdType.MESH)

    def blocks(q, ph, away):
        idx = [slice(None)] * 3
        for i in range(ph):
            idx[SPLIT[q][i]] = pos[SPLIT[q][i]]
        a = SPLIT[q][ph]
        idx[a] = 1 - pos[a] if away else pos[a]
        return tuple(idx)

    def rs_copy(s, q, ph):
        l0, ln = LANES[q]
        lanes = pl.ds(l0, ln)
        src = snd_ref.at[(s % N_SND,) + blocks(q, ph, True) + (slice(None), lanes)]
        rs = s % N_RCV
        dst = (r1_ref.at[rs, :, :, :, lanes], r2_ref.at[rs, :, :, lanes], r3_ref.at[rs, :, lanes])[ph]
        return pltpu.make_async_remote_copy(
            src_ref=src, dst_ref=dst, send_sem=rs_ssem.at[s % N_SND, q, ph], recv_sem=rs_rsem.at[s, q, ph],
            device_id=(flip(me, 8 >> SPLIT[q][ph]),), device_id_type=pl.DeviceIdType.MESH)

    def fin_copy(o):
        return pltpu.make_async_remote_copy(
            src_ref=fin_snd, dst_ref=fin_rcv.at[me], send_sem=fin_ssem.at[o],
            recv_sem=fin_rsem.at[o], device_id=((me + o) % N_DEV,), device_id_type=pl.DeviceIdType.MESH)

    e_copy = pltpu.make_async_copy(e_hbm, e_ref.at[:, 0:dim], lsem.at[4])
    xo_copy = pltpu.make_async_copy(x_hbm.at[chip, core], xo_ref, lsem.at[5])
    e_copy.start()
    x_copy(0).start()

    barrier = pltpu.get_barrier_semaphore()
    for o in range(1, N_DEV):
        pl.semaphore_signal(barrier, inc=1, device_id=((me + o) % N_DEV,), device_id_type=pl.DeviceIdType.MESH)

    inv_total = 1.0 / jnp.sum(jnp.where(lab_ref[...] >= 0, 1.0, 0.0))
    tgt_ref[...] = jnp.zeros_like(tgt_ref)
    dg8_ref[...] = jnp.zeros_like(dg8_ref)
    gain = gain_ref[...]

    def norm_rows(xv):
        xf = xv.astype(jnp.float32)
        inv = lax.rsqrt(jnp.mean(xf * xf, axis=-1, keepdims=True) + NORM_EPS)
        return xf, inv

    def norm_block(slot, k, c):
        xf, inv = norm_rows(x_ref[k, c])
        h_ref[slot, k, c] = ((xf * inv) * gain).astype(jnp.bfloat16)

    for t in range(2):
        x_copy(t).wait()

        @pl.loop(0, TC // TB)
        def _(i, t=t):
            norm_block(t, i // 8, i % 8)

        if t == 0:
            x_copy(1).start()
            xo_copy.start()
    xo_copy.wait()
    pl.semaphore_wait(barrier, N_DEV - 1)
    e_copy.wait()

    def phase_a(t):
        slot = t % 2
        @pl.when(t < N_XLA)
        def _():
            h_copy(t).start()

        @pl.when(t == N_XLA)
        def _():
            ht_copy().start()

        @pl.when((t > 0) & (t < N_STEP - 1))
        def _():
            x_copy(t + 1).start()

        h_val = h_ref[t % 2].reshape(TC, dim)
        m8 = None
        for idx, (r0, rn) in enumerate(A_TILES):
            z = lax.dot_general(e_ref[r0:r0 + rn, 0:dim], h_val, (((1,), (1,)), ((), ())),
                                preferred_element_type=jnp.float32)
            if idx == len(A_TILES) - 1:
                rid = lax.broadcasted_iota(jnp.int32, (rn, TC), 0) + (r0 + v0)
                z = jnp.where(rid < VOCAB_REAL, z, NEG)
            z_ref[slot, r0:r0 + rn, :] = z
            zr = z.reshape(rn // 8, 8, TC)
            mt = jnp.max(zr, axis=0)
            if m8 is None:
                mn = mt
                s8 = jnp.sum(jnp.exp2((zr - mn[None]) * C2), axis=0)
            else:
                mn = jnp.maximum(m8, mt)
                s8 = s8 * jnp.exp2((m8 - mn) * C2) + jnp.sum(jnp.exp2((zr - mn[None]) * C2), axis=0)
            m8 = mn
        mx = jnp.max(m8, axis=0, keepdims=True)
        sm = jnp.sum(s8 * jnp.exp2((m8 - mx) * C2), axis=0, keepdims=True)

        @pl.when(t > 0)
        def _():
            for o in range(1, N_DEV):
                st_copy(t - 1, o).wait_send()

        for i in range(4):
            st_snd[t, i:i + 1, :] = mx[:, 128 * i:128 * (i + 1)]
            st_snd[t, 4 + i:5 + i, :] = sm[:, 128 * i:128 * (i + 1)]
        st_rcv[t, me] = st_snd[t]
        for o in range(1, N_DEV):
            st_copy(t, o).start()

    def phase_b(t):
        slot = t % 2
        for o in range(1, N_DEV):
            st_copy(t, o).wait_recv()
        mx = st_rcv[t, 0, 0:4, :]
        for i in range(1, N_DEV):
            mx = jnp.maximum(mx, st_rcv[t, i, 0:4, :])
        sm = jnp.zeros_like(mx)
        for i in range(N_DEV):
            sm = sm + st_rcv[t, i, 4:8, :] * jnp.exp2((st_rcv[t, i, 0:4, :] - mx) * C2)
        lse = mx * (1.0 / LOGIT_SCALE) + jnp.log(sm)
        inv_s = 1.0 / sm
        lse_row = jnp.concatenate([lse[i:i + 1] for i in range(4)], axis=1)
        lse_ref[t] = jnp.where(lab_ref[t] >= 0, lse_row, 0.0)
        m8_ref[...] = jnp.concatenate([mx[i:i + 1] for i in range(4)], axis=1)
        s8_ref[...] = jnp.concatenate([inv_s[i:i + 1] for i in range(4)], axis=1)

        @pl.when(t > 0)
        def _():
            dz_save_wait(t - 1)
            d2d_copy(t - 1).wait_send()

        @pl.when(t < N_XLA)
        def _():
            h_copy(t).wait()

        @pl.when(t == N_XLA)
        def _():
            ht_copy().wait()

        @pl.when(t < N_STEP - 2)
        def _():
            x_copy(t + 2).wait()

        spare = (t + 2) // N_STEP
        h_slot = (t % 2) * (1 - spare) + 2 * spare

        @pl.loop(0, 2)
        def _(hf):
            off = pl.multiple_of(((hf + 1 + core) % 2) * HALF, HALF)
            cols = pl.ds(off, HALF)
            mrow = m8_ref[:, cols]
            irow = s8_ref[:, cols]
            lab = lab_ref[t, :, cols]
            mk = jnp.where(lab >= 0, 1.0, 0.0)
            wrow = mk * inv_total
            lab = lab - v0
            tg = jnp.zeros((8, HALF), jnp.float32)
            for idx, (r0, rn) in enumerate(B_TILES):
                z = z_ref[slot, r0:r0 + rn, cols]
                p = jnp.exp2((z - mrow) * C2) * irow
                isl = lax.broadcasted_iota(jnp.int32, (rn, HALF), 0) == (lab - r0)
                dz = (jnp.where(isl, p - 1.0, p) * wrow).astype(jnp.bfloat16)
                tg = tg + jnp.sum(jnp.where(isl, z, 0.0).reshape(rn // 8, 8, HALF), axis=0)
                dz_ref[r0:r0 + rn, cols] = dz
                for c in range(8 * idx // len(B_TILES), 8 * (idx + 1) // len(B_TILES)):
                    norm_block(h_slot, hf, c)
                part = lax.dot_general(dz, e_ref[r0:r0 + rn, 0:dim], (((0,), (0,)), ((), ())),
                                       preferred_element_type=jnp.float32)
                if idx == 0:
                    dh_ref[hf] = part
                else:
                    dh_ref[hf] += part
            tgt_ref[...] += tg * mk

            @pl.when(hf == 0)
            def _():
                d2d_copy(t).start()

                @pl.when(t > 0)
                def _():
                    rs_advance(t - 1, 1)

        dz_save(t)
        d2d_copy(t).wait_recv()

    def rs_begin(s):
        slot = s % N_SND

        @pl.when(s >= N_SND)
        def _():
            for q in range(3):
                for ph in range(3):
                    rs_copy(s - N_SND, q, ph).wait_send()

        for c in range(8):
            rows = pl.ds(c * TB, TB)
            snd_ref[slot, c // 4, (c // 2) % 2, c % 2] = dh_ref[1, rows, :] + d2d_ref[s % 2, rows, :]
        for q in range(3):
            rs_copy(s, q, 0).start()

    def rs_advance(s, ph):
        slot = s % N_SND
        for q in range(3):
            rs_copy(s, q, ph - 1).wait_recv()
            l0, ln = LANES[q]
            lanes = slice(l0, l0 + ln)
            base = blocks(q, ph - 1, False)
            free = [i for i in range(3) if isinstance(base[i], slice)]
            for n in range(2 ** len(free)):
                bits = [(n >> k) & 1 for k in reversed(range(len(free)))]
                idx = list(base)
                for i, bit in zip(free, bits):
                    idx[i] = bit
                rcv = (r1_ref if ph == 1 else r2_ref)[(s % N_RCV, *bits, slice(None), lanes)]
                loc = (slot, *idx, slice(None), lanes)
                snd_ref[loc] = snd_ref[loc] + rcv
            rs_copy(s, q, ph).start()

    def rs_finish(s):
        for q in range(3):
            rs_copy(s, q, 2).wait_recv()

        @pl.loop(0, TB // 8)
        def _(i):
            rows = pl.ds(pl.multiple_of(i * 8, 8), 8)
            acc = (snd_ref[s % N_SND, pos[0], pos[1], pos[2], rows, :] + r3_ref[s % N_RCV, rows, :]) * (1.0 / LOGIT_SCALE)
            xf, inv = norm_rows(xo_ref[s, rows, :])
            xh = xf * inv
            u = acc * gain
            dx_ref[pl.ds(pl.multiple_of(s * TB + i * 8, 8), 8), :] = inv * (
                u - xh * jnp.mean(u * xh, axis=-1, keepdims=True))
            dg8_ref[...] += acc * xh

    @pl.loop(0, N_STEP + 1)
    def _(t):
        @pl.when(t < N_STEP)
        def _():
            phase_a(t)

        @pl.when(t > 3)
        def _():
            rs_finish(t - 4)

        @pl.when(t > 2)
        def _():
            rs_advance(t - 3, 2)

        @pl.when(t > 0)
        def _():
            phase_b(t - 1)
            rs_begin(t - 1)

    loads = [pltpu.make_async_copy(dzt_hbm.at[i], e_ref.at[:, i * TC:(i + 1) * TC], lsem.at[i]) for i in range(2)]
    loads.append(pltpu.make_async_copy(ht_hbm, x_ref, lsem.at[2]))
    for c in loads:
        c.start()
    rs_finish(N_STEP - 3)
    rs_advance(N_STEP - 2, 2)
    for c in loads:
        c.wait()

    @pl.loop(0, dim // TC)
    def _(n):
        @pl.when(n > 1)
        def _():
            part_copy(n - 2).wait()

        cols = pl.ds(pl.multiple_of(n * TC, TC), TC)
        for r0, rn in A_TILES:
            acc = None
            for lhs, rhs in ((dz_ref[r0:r0 + rn, :], h_ref[(N_STEP - 1) % 2, :, :, :, cols]),
                             (e_ref[r0:r0 + rn, TC:2 * TC], h_ref[(N_STEP - 2) % 2, :, :, :, cols]),
                             (e_ref[r0:r0 + rn, 0:TC], x_ref[:, :, :, cols])):
                part = jnp.dot(lhs, rhs.reshape(TC, TC), preferred_element_type=jnp.float32)
                acc = part if acc is None else acc + part
            z_ref[n % 2, r0:r0 + rn, :] = acc
        part_copy(n).start()

        @pl.when(n == 1)
        def _():
            rs_advance(N_STEP - 1, 1)
            rs_finish(N_STEP - 2)

        @pl.when(n == 2)
        def _():
            rs_advance(N_STEP - 1, 2)

    rs_finish(N_STEP - 1)

    dg = jnp.sum(dg8_ref[...], axis=0, keepdims=True)
    for i in range(dim // 128):
        fin_snd[i:i + 1, :] = dg[:, 128 * i:128 * (i + 1)]
    tg = jnp.sum(tgt_ref[...], axis=0, keepdims=True)
    fin_snd[16:24, :] = jnp.broadcast_to(tg[:, 0:128] + tg[:, 128:256], (8, 128))
    fin_rcv[me] = fin_snd[...]
    for o in range(1, N_DEV):
        fin_copy(o).start()
    for o in range(1, N_DEV):
        st_copy(N_STEP - 1, o).wait_send()
        fin_copy(o).wait()
    tot = fin_rcv[0]
    for i in range(1, N_DEV):
        tot = tot + fin_rcv[i]
    dg_ref[...] = tot[0:16, :]
    lse_sum = jnp.sum(lse_ref[...])
    tgt_sum = jnp.sum(tot[16:17, :]) * (1.0 / LOGIT_SCALE)
    loss_ref[...] = jnp.broadcast_to((lse_sum - tgt_sum) * inv_total, (1, 1))

    for s in range(N_STEP - N_SND, N_STEP):
        for q in range(3):
            for ph in range(3):
                rs_copy(s, q, ph).wait_send()
    part_copy(2).wait()
    part_copy(3).wait()
    d2d_copy(N_STEP - 1).wait_send()


def solution(mesh):
    axis = mesh.axis_names[0]

    def local_step(residual, labels, loss_mask, norm_gain, table_shard):
        tokens, dim = residual.shape
        v_rows = table_shard.shape[0]
        by_step = lambda a: a.reshape(8, 2, N_STEP, TB).transpose(2, 1, 0, 3)
        any_spec = pl.BlockSpec(memory_space=pl.ANY)
        vmem = pl.BlockSpec(memory_space=pltpu.VMEM)
        f32, bf16 = jnp.float32, jnp.bfloat16
        dma = pltpu.SemaphoreType.DMA
        dz, h, _, _, part, dx, dg, loss = pl.pallas_call(
            functools.partial(kernel, axis, v_rows, dim),
            out_shape=(
                jax.ShapeDtypeStruct((v_rows, N_XLA * TC), bf16),
                jax.ShapeDtypeStruct((N_XLA, 2, 8, TB, dim), bf16),
                jax.ShapeDtypeStruct((2, v_rows, TC), bf16),
                jax.ShapeDtypeStruct((2, 8, TB, dim), bf16),
                jax.ShapeDtypeStruct((v_rows, dim), f32),
                jax.ShapeDtypeStruct((HALF, dim), f32),
                jax.ShapeDtypeStruct((16, 128), f32),
                jax.ShapeDtypeStruct((1, 1), f32),
            ),
            in_specs=[any_spec, vmem, vmem, any_spec],
            out_specs=(any_spec, any_spec, any_spec, any_spec, any_spec, vmem, vmem, vmem),
            scratch_shapes=[
                pltpu.VMEM((v_rows, dim + PAD), bf16),
                pltpu.VMEM((2, v_rows, TC), f32),
                pltpu.VMEM((2, 8, TB, dim), bf16),
                pltpu.VMEM((N_STEP, TB, dim), bf16),
                pltpu.VMEM((3, 2, 8, TB, dim), bf16),
                pltpu.VMEM((v_rows, TC), bf16),
                pltpu.VMEM((2, HALF, dim), f32),
                pltpu.VMEM((2, HALF, dim), f32),
                pltpu.VMEM((N_SND, 2, 2, 2, TB, dim), f32),
                pltpu.VMEM((N_RCV, 2, 2, TB, dim), f32),
                pltpu.VMEM((N_RCV, 2, TB, dim), f32),
                pltpu.VMEM((N_RCV, TB, dim), f32),
                pltpu.VMEM((N_STEP, 8, 128), f32),
                pltpu.VMEM((N_STEP, N_DEV, 8, 128), f32),
                pltpu.VMEM((N_STEP, 1, TC), f32),
                pltpu.VMEM((8, HALF), f32),
                pltpu.VMEM((8, dim), f32),
                pltpu.VMEM((1, TC), f32),
                pltpu.VMEM((1, TC), f32),
                pltpu.VMEM((24, 128), f32),
                pltpu.VMEM((N_DEV, 24, 128), f32),
                dma((N_DEV,)), dma((N_STEP, N_DEV)), dma((1,)), dma((2,)),
                dma((N_SND, 3, 3)), dma((N_STEP, 3, 3)), dma((N_DEV,)), dma((N_DEV,)), dma((10,)),
            ],
            compiler_params=pltpu.CompilerParams(
                collective_id=0, has_side_effects=True, vmem_limit_bytes=67043328),
            name="xent_fused",
        )(residual.reshape(8, 2, N_STEP, TB, dim), by_step(jnp.where(loss_mask > 0, labels, -1)).reshape(N_STEP, 1, TC),
          norm_gain.reshape(1, dim), table_shard)
        d_embed = (jnp.dot(dz, h.reshape(N_XLA * TC, dim), preferred_element_type=f32) + part) / LOGIT_SCALE
        return loss.reshape(()), dx, d_embed, dg.reshape(dim)

    return jax.shard_map(local_step, mesh=mesh, in_specs=(P(), P(), P(), P(), P(axis, None)),
                         out_specs=(P(), P(axis, None), P(axis, None), P()), check_vma=False)
```

```python
import functools

import jax
import jax.numpy as jnp
from jax import lax
from jax.experimental import pallas as pl
from jax.experimental.pallas import tpu as pltpu
from jax.sharding import PartitionSpec as P

VOCAB_REAL = 49155
LOGIT_SCALE = 6.0
NORM_EPS = 1e-6
LOG2E = 1.4426950408889634
C2 = LOG2E / LOGIT_SCALE
NEG = -3e38
N_DEV = 16
N_STEP = 8
TC = 512
HALF = 256
LANES = ((0, 768), (768, 640), (1408, 640))
SPLIT = ((2, 1, 0), (1, 0, 2), (0, 2, 1))
N_SND = 3
N_RCV = 4
TB = 32
N_XLA = 5
PAD = 128


def flip(i, b):
    return i + b - 2 * b * ((i // b) % 2)


def v_tiles(rows, step):
    n = rows // step
    out = [(i * step, step) for i in range(n)]
    rest = rows - n * step
    if rest:
        out[-1] = (out[-1][0], step + rest)
    return out


def kernel(axis, v_rows, dim,
           x_hbm, lab_ref, gain_ref, e_hbm,
           dz_hbm, h_hbm, dzt_hbm, ht_hbm, part_hbm, dx_ref, dg_ref, loss_ref,
           e_ref, z_ref, x_ref, xo_ref, h_ref, dz_ref, dh_ref, d2d_ref, snd_ref, r1_ref, r2_ref, r3_ref,
           st_snd, st_rcv, lse_ref, tgt_ref, dg8_ref, m8_ref, s8_ref, fin_snd, fin_rcv,
           st_ssem, st_rsem, d2d_ssem, d2d_rsem, rs_ssem, rs_rsem, fin_ssem, fin_rsem, lsem):
    me = lax.axis_index(axis)
    chip = me // 2
    core = me % 2
    pos = (chip // 4, (chip // 2) % 2, chip % 2)
    v0 = me * v_rows
    A_TILES = v_tiles(v_rows - 288, 400) + [(v_rows - 288, 288)]
    C_TILES = v_tiles(v_rows, 384)
    B_TILES = v_tiles(v_rows, 768)

    class Group:
        def __init__(self, copies):
            self.copies = copies

        def start(self):
            for c in self.copies:
                c.start()

        def wait(self):
            for c in self.copies:
                c.wait()

    def x_copy(t):
        return Group([pltpu.make_async_copy(x_hbm.at[:, k, t], x_ref.at[k], lsem.at[k]) for k in range(2)])

    def h_copy(t):
        return pltpu.make_async_copy(h_ref.at[t % 2], h_hbm.at[t], lsem.at[8 + t % 2])

    def dz_copy(t):
        return pltpu.make_async_copy(dz_ref, dz_hbm.at[:, pl.ds(pl.multiple_of(t * TC, TC), TC)], lsem.at[3])

    def ht_copy():
        return pltpu.make_async_copy(h_ref.at[N_XLA % 2], ht_hbm, lsem.at[8 + N_XLA % 2])

    def dzt_copy(t):
        return pltpu.make_async_copy(dz_ref, dzt_hbm.at[t - N_XLA], lsem.at[3])

    def dz_save(t):
        @pl.when(t < N_XLA)
        def _():
            dz_copy(t).start()

        @pl.when((t >= N_XLA) & (t < N_STEP - 1))
        def _():
            dzt_copy(t).start()

    def dz_save_wait(t):
        @pl.when(t < N_XLA)
        def _():
            dz_copy(t).wait()

        @pl.when(t >= N_XLA)
        def _():
            dzt_copy(t).wait()

    def part_copy(n):
        return pltpu.make_async_copy(
            z_ref.at[n % 2], part_hbm.at[:, pl.ds(pl.multiple_of(n * TC, TC), TC)], lsem.at[6 + n % 2])

    def st_copy(t, o):
        return pltpu.make_async_remote_copy(
            src_ref=st_snd.at[t], dst_ref=st_rcv.at[t, me], send_sem=st_ssem.at[o],
            recv_sem=st_rsem.at[t, o], device_id=((me + o) % N_DEV,), device_id_type=pl.DeviceIdType.MESH)

    def d2d_copy(t):
        return pltpu.make_async_remote_copy(
            src_ref=dh_ref.at[0], dst_ref=d2d_ref.at[t % 2], send_sem=d2d_ssem.at[0],
            recv_sem=d2d_rsem.at[t % 2], device_id=(flip(me, 1),), device_id_type=pl.DeviceIdType.MESH)

    def blocks(q, ph, away):
        idx = [slice(None)] * 3
        for i in range(ph):
            idx[SPLIT[q][i]] = pos[SPLIT[q][i]]
        a = SPLIT[q][ph]
        idx[a] = 1 - pos[a] if away else pos[a]
        return tuple(idx)

    def rs_copy(s, q, ph):
        l0, ln = LANES[q]
        lanes = pl.ds(l0, ln)
        src = snd_ref.at[(s % N_SND,) + blocks(q, ph, True) + (slice(None), lanes)]
        rs = s % N_RCV
        dst = (r1_ref.at[rs, :, :, :, lanes], r2_ref.at[rs, :, :, lanes], r3_ref.at[rs, :, lanes])[ph]
        return pltpu.make_async_remote_copy(
            src_ref=src, dst_ref=dst, send_sem=rs_ssem.at[s % N_SND, q, ph], recv_sem=rs_rsem.at[s, q, ph],
            device_id=(flip(me, 8 >> SPLIT[q][ph]),), device_id_type=pl.DeviceIdType.MESH)

    def fin_copy(o):
        return pltpu.make_async_remote_copy(
            src_ref=fin_snd, dst_ref=fin_rcv.at[me], send_sem=fin_ssem.at[o],
            recv_sem=fin_rsem.at[o], device_id=((me + o) % N_DEV,), device_id_type=pl.DeviceIdType.MESH)

    e_copy = pltpu.make_async_copy(e_hbm, e_ref.at[:, 0:dim], lsem.at[4])
    xo_copy = pltpu.make_async_copy(x_hbm.at[chip, core], xo_ref, lsem.at[5])
    e_copy.start()
    x_copy(0).start()

    barrier = pltpu.get_barrier_semaphore()
    for o in range(1, N_DEV):
        pl.semaphore_signal(barrier, inc=1, device_id=((me + o) % N_DEV,), device_id_type=pl.DeviceIdType.MESH)

    inv_total = 1.0 / jnp.sum(jnp.where(lab_ref[...] >= 0, 1.0, 0.0))
    tgt_ref[...] = jnp.zeros_like(tgt_ref)
    dg8_ref[...] = jnp.zeros_like(dg8_ref)
    gain = gain_ref[...]

    def norm_rows(xv):
        xf = xv.astype(jnp.float32)
        inv = lax.rsqrt(jnp.mean(xf * xf, axis=-1, keepdims=True) + NORM_EPS)
        return xf, inv

    def norm_block(slot, k, c):
        xf, inv = norm_rows(x_ref[k, c])
        h_ref[slot, k, c] = ((xf * inv) * gain).astype(jnp.bfloat16)

    for t in range(2):
        x_copy(t).wait()

        @pl.loop(0, TC // TB)
        def _(i, t=t):
            norm_block(t, i // 8, i % 8)

        if t == 0:
            x_copy(1).start()
            xo_copy.start()
    xo_copy.wait()
    pl.semaphore_wait(barrier, N_DEV - 1)
    e_copy.wait()

    def phase_a(t):
        slot = t % 2
        @pl.when(t < N_XLA)
        def _():
            h_copy(t).start()

        @pl.when(t == N_XLA)
        def _():
            ht_copy().start()

        @pl.when((t > 0) & (t < N_STEP - 1))
        def _():
            x_copy(t + 1).start()

        h_val = h_ref[t % 2].reshape(TC, dim)
        m8 = None
        for idx, (r0, rn) in enumerate(A_TILES):
            z = lax.dot_general(e_ref[r0:r0 + rn, 0:dim], h_val, (((1,), (1,)), ((), ())),
                                preferred_element_type=jnp.float32)
            if idx == len(A_TILES) - 1:
                rid = lax.broadcasted_iota(jnp.int32, (rn, TC), 0) + (r0 + v0)
                z = jnp.where(rid < VOCAB_REAL, z, NEG)
            z_ref[slot, r0:r0 + rn, :] = z
            zr = z.reshape(rn // 8, 8, TC)
            mt = jnp.max(zr, axis=0)
            if m8 is None:
                mn = mt
                s8 = jnp.sum(jnp.exp2((zr - mn[None]) * C2), axis=0)
            else:
                mn = jnp.maximum(m8, mt)
                s8 = s8 * jnp.exp2((m8 - mn) * C2) + jnp.sum(jnp.exp2((zr - mn[None]) * C2), axis=0)
            m8 = mn
        mx = jnp.max(m8, axis=0, keepdims=True)
        sm = jnp.sum(s8 * jnp.exp2((m8 - mx) * C2), axis=0, keepdims=True)

        @pl.when(t > 0)
        def _():
            for o in range(1, N_DEV):
                st_copy(t - 1, o).wait_send()

        for i in range(4):
            st_snd[t, i:i + 1, :] = mx[:, 128 * i:128 * (i + 1)]
            st_snd[t, 4 + i:5 + i, :] = sm[:, 128 * i:128 * (i + 1)]
        st_rcv[t, me] = st_snd[t]
        for o in range(1, N_DEV):
            st_copy(t, o).start()

    def phase_b(t):
        slot = t % 2
        for o in range(1, N_DEV):
            st_copy(t, o).wait_recv()
        mx = st_rcv[t, 0, 0:4, :]
        for i in range(1, N_DEV):
            mx = jnp.maximum(mx, st_rcv[t, i, 0:4, :])
        sm = jnp.zeros_like(mx)
        for i in range(N_DEV):
            sm = sm + st_rcv[t, i, 4:8, :] * jnp.exp2((st_rcv[t, i, 0:4, :] - mx) * C2)
        lse = mx * (1.0 / LOGIT_SCALE) + jnp.log(sm)
        inv_s = 1.0 / sm
        lse_row = jnp.concatenate([lse[i:i + 1] for i in range(4)], axis=1)
        lse_ref[t] = jnp.where(lab_ref[t] >= 0, lse_row, 0.0)
        m8_ref[...] = jnp.concatenate([mx[i:i + 1] for i in range(4)], axis=1)
        s8_ref[...] = jnp.concatenate([inv_s[i:i + 1] for i in range(4)], axis=1)

        @pl.when(t > 0)
        def _():
            dz_save_wait(t - 1)
            d2d_copy(t - 1).wait_send()

        @pl.when(t < N_XLA)
        def _():
            h_copy(t).wait()

        @pl.when(t == N_XLA)
        def _():
            ht_copy().wait()

        @pl.when(t < N_STEP - 2)
        def _():
            x_copy(t + 2).wait()

        spare = (t + 2) // N_STEP
        h_slot = (t % 2) * (1 - spare) + 2 * spare

        @pl.loop(0, 2)
        def _(hf):
            off = pl.multiple_of(((hf + 1 + core) % 2) * HALF, HALF)
            cols = pl.ds(off, HALF)
            mrow = m8_ref[:, cols]
            irow = s8_ref[:, cols]
            lab = lab_ref[t, :, cols]
            mk = jnp.where(lab >= 0, 1.0, 0.0)
            wrow = mk * inv_total
            lab = lab - v0
            tg = jnp.zeros((8, HALF), jnp.float32)
            for idx, (r0, rn) in enumerate(B_TILES):
                z = z_ref[slot, r0:r0 + rn, cols]
                p = jnp.exp2((z - mrow) * C2) * irow
                isl = lax.broadcasted_iota(jnp.int32, (rn, HALF), 0) == (lab - r0)
                dz = (jnp.where(isl, p - 1.0, p) * wrow).astype(jnp.bfloat16)
                tg = tg + jnp.sum(jnp.where(isl, z, 0.0).reshape(rn // 8, 8, HALF), axis=0)
                dz_ref[r0:r0 + rn, cols] = dz
                for c in range(8 * idx // len(B_TILES), 8 * (idx + 1) // len(B_TILES)):
                    norm_block(h_slot, hf, c)
                part = lax.dot_general(dz, e_ref[r0:r0 + rn, 0:dim], (((0,), (0,)), ((), ())),
                                       preferred_element_type=jnp.float32)
                if idx == 0:
                    dh_ref[hf] = part
                else:
                    dh_ref[hf] += part
            tgt_ref[...] += tg * mk

            @pl.when(hf == 0)
            def _():
                d2d_copy(t).start()

                @pl.when(t > 0)
                def _():
                    rs_advance(t - 1, 1)

        dz_save(t)
        d2d_copy(t).wait_recv()

    def rs_begin(s):
        slot = s % N_SND

        @pl.when(s >= N_SND)
        def _():
            for q in range(3):
                for ph in range(3):
                    rs_copy(s - N_SND, q, ph).wait_send()

        for c in range(8):
            rows = pl.ds(c * TB, TB)
            snd_ref[slot, c // 4, (c // 2) % 2, c % 2] = dh_ref[1, rows, :] + d2d_ref[s % 2, rows, :]
        for q in range(3):
            rs_copy(s, q, 0).start()

    def rs_advance(s, ph):
        slot = s % N_SND
        for q in range(3):
            rs_copy(s, q, ph - 1).wait_recv()
            l0, ln = LANES[q]
            lanes = slice(l0, l0 + ln)
            base = blocks(q, ph - 1, False)
            free = [i for i in range(3) if isinstance(base[i], slice)]
            for n in range(2 ** len(free)):
                bits = [(n >> k) & 1 for k in reversed(range(len(free)))]
                idx = list(base)
                for i, bit in zip(free, bits):
                    idx[i] = bit
                rcv = (r1_ref if ph == 1 else r2_ref)[(s % N_RCV, *bits, slice(None), lanes)]
                loc = (slot, *idx, slice(None), lanes)
                snd_ref[loc] = snd_ref[loc] + rcv
            rs_copy(s, q, ph).start()

    def rs_finish(s):
        for q in range(3):
            rs_copy(s, q, 2).wait_recv()

        @pl.loop(0, TB // 8)
        def _(i):
            rows = pl.ds(pl.multiple_of(i * 8, 8), 8)
            acc = (snd_ref[s % N_SND, pos[0], pos[1], pos[2], rows, :] + r3_ref[s % N_RCV, rows, :]) * (1.0 / LOGIT_SCALE)
            xf, inv = norm_rows(xo_ref[s, rows, :])
            xh = xf * inv
            u = acc * gain
            dx_ref[pl.ds(pl.multiple_of(s * TB + i * 8, 8), 8), :] = inv * (
                u - xh * jnp.mean(u * xh, axis=-1, keepdims=True))
            dg8_ref[...] += acc * xh

    @pl.loop(0, N_STEP + 1)
    def _(t):
        @pl.when(t < N_STEP)
        def _():
            phase_a(t)

        @pl.when(t > 3)
        def _():
            rs_finish(t - 4)

        @pl.when(t > 2)
        def _():
            rs_advance(t - 3, 2)

        @pl.when(t > 0)
        def _():
            phase_b(t - 1)
            rs_begin(t - 1)

    loads = [pltpu.make_async_copy(dzt_hbm.at[i], e_ref.at[:, i * TC:(i + 1) * TC], lsem.at[i]) for i in range(2)]
    loads.append(pltpu.make_async_copy(ht_hbm, x_ref, lsem.at[2]))
    for c in loads:
        c.start()
    rs_finish(N_STEP - 3)
    rs_advance(N_STEP - 2, 2)
    for c in loads:
        c.wait()

    @pl.loop(0, dim // TC)
    def _(n):
        @pl.when(n > 1)
        def _():
            part_copy(n - 2).wait()

        cols = pl.ds(pl.multiple_of(n * TC, TC), TC)
        for r0, rn in C_TILES:
            acc = None
            for lhs, rhs in ((dz_ref[r0:r0 + rn, :], h_ref[(N_STEP - 1) % 2, :, :, :, cols]),
                             (e_ref[r0:r0 + rn, TC:2 * TC], h_ref[(N_STEP - 2) % 2, :, :, :, cols]),
                             (e_ref[r0:r0 + rn, 0:TC], x_ref[:, :, :, cols])):
                part = jnp.dot(lhs, rhs.reshape(TC, TC), preferred_element_type=jnp.float32)
                acc = part if acc is None else acc + part
            z_ref[n % 2, r0:r0 + rn, :] = acc
        part_copy(n).start()

        @pl.when(n == 1)
        def _():
            rs_advance(N_STEP - 1, 1)
            rs_finish(N_STEP - 2)

        @pl.when(n == 2)
        def _():
            rs_advance(N_STEP - 1, 2)

    rs_finish(N_STEP - 1)

    dg = jnp.sum(dg8_ref[...], axis=0, keepdims=True)
    for i in range(dim // 128):
        fin_snd[i:i + 1, :] = dg[:, 128 * i:128 * (i + 1)]
    tg = jnp.sum(tgt_ref[...], axis=0, keepdims=True)
    fin_snd[16:24, :] = jnp.broadcast_to(tg[:, 0:128] + tg[:, 128:256], (8, 128))
    fin_rcv[me] = fin_snd[...]
    for o in range(1, N_DEV):
        fin_copy(o).start()
    for o in range(1, N_DEV):
        st_copy(N_STEP - 1, o).wait_send()
        fin_copy(o).wait()
    tot = fin_rcv[0]
    for i in range(1, N_DEV):
        tot = tot + fin_rcv[i]
    dg_ref[...] = tot[0:16, :]
    lse_sum = jnp.sum(lse_ref[...])
    tgt_sum = jnp.sum(tot[16:17, :]) * (1.0 / LOGIT_SCALE)
    loss_ref[...] = jnp.broadcast_to((lse_sum - tgt_sum) * inv_total, (1, 1))

    for s in range(N_STEP - N_SND, N_STEP):
        for q in range(3):
            for ph in range(3):
                rs_copy(s, q, ph).wait_send()
    part_copy(2).wait()
    part_copy(3).wait()
    d2d_copy(N_STEP - 1).wait_send()


def solution(mesh):
    axis = mesh.axis_names[0]

    def local_step(residual, labels, loss_mask, norm_gain, table_shard):
        tokens, dim = residual.shape
        v_rows = table_shard.shape[0]
        by_step = lambda a: a.reshape(8, 2, N_STEP, TB).transpose(2, 1, 0, 3)
        any_spec = pl.BlockSpec(memory_space=pl.ANY)
        vmem = pl.BlockSpec(memory_space=pltpu.VMEM)
        f32, bf16 = jnp.float32, jnp.bfloat16
        dma = pltpu.SemaphoreType.DMA
        dz, h, _, _, part, dx, dg, loss = pl.pallas_call(
            functools.partial(kernel, axis, v_rows, dim),
            out_shape=(
                jax.ShapeDtypeStruct((v_rows, N_XLA * TC), bf16),
                jax.ShapeDtypeStruct((N_XLA, 2, 8, TB, dim), bf16),
                jax.ShapeDtypeStruct((2, v_rows, TC), bf16),
                jax.ShapeDtypeStruct((2, 8, TB, dim), bf16),
                jax.ShapeDtypeStruct((v_rows, dim), f32),
                jax.ShapeDtypeStruct((HALF, dim), f32),
                jax.ShapeDtypeStruct((16, 128), f32),
                jax.ShapeDtypeStruct((1, 1), f32),
            ),
            in_specs=[any_spec, vmem, vmem, any_spec],
            out_specs=(any_spec, any_spec, any_spec, any_spec, any_spec, vmem, vmem, vmem),
            scratch_shapes=[
                pltpu.VMEM((v_rows, dim + PAD), bf16),
                pltpu.VMEM((2, v_rows, TC), f32),
                pltpu.VMEM((2, 8, TB, dim), bf16),
                pltpu.VMEM((N_STEP, TB, dim), bf16),
                pltpu.VMEM((3, 2, 8, TB, dim), bf16),
                pltpu.VMEM((v_rows, TC), bf16),
                pltpu.VMEM((2, HALF, dim), f32),
                pltpu.VMEM((2, HALF, dim), f32),
                pltpu.VMEM((N_SND, 2, 2, 2, TB, dim), f32),
                pltpu.VMEM((N_RCV, 2, 2, TB, dim), f32),
                pltpu.VMEM((N_RCV, 2, TB, dim), f32),
                pltpu.VMEM((N_RCV, TB, dim), f32),
                pltpu.VMEM((N_STEP, 8, 128), f32),
                pltpu.VMEM((N_STEP, N_DEV, 8, 128), f32),
                pltpu.VMEM((N_STEP, 1, TC), f32),
                pltpu.VMEM((8, HALF), f32),
                pltpu.VMEM((8, dim), f32),
                pltpu.VMEM((1, TC), f32),
                pltpu.VMEM((1, TC), f32),
                pltpu.VMEM((24, 128), f32),
                pltpu.VMEM((N_DEV, 24, 128), f32),
                dma((N_DEV,)), dma((N_STEP, N_DEV)), dma((1,)), dma((2,)),
                dma((N_SND, 3, 3)), dma((N_STEP, 3, 3)), dma((N_DEV,)), dma((N_DEV,)), dma((10,)),
            ],
            compiler_params=pltpu.CompilerParams(
                collective_id=0, has_side_effects=True, vmem_limit_bytes=67043328),
            name="xent_fused",
        )(residual.reshape(8, 2, N_STEP, TB, dim), by_step(jnp.where(loss_mask > 0, labels, -1)).reshape(N_STEP, 1, TC),
          norm_gain.reshape(1, dim), table_shard)
        d_embed = (jnp.dot(dz, h.reshape(N_XLA * TC, dim), preferred_element_type=f32) + part) / LOGIT_SCALE
        return loss.reshape(()), dx, d_embed, dg.reshape(dim)

    return jax.shard_map(local_step, mesh=mesh, in_specs=(P(), P(), P(), P(), P(axis, None)),
                         out_specs=(P(), P(axis, None), P(axis, None), P()), check_vma=False)
```
